128 devices in a mesh: slab: 4 (over x), blk: 32 (over y, z, core).
Axes of the slice: x: 4, y: 4, z: 4, core: 2. Of those that a mesh axis runs over, the one named last changes fastest.
Arguments:
- amplitudes: bfloat16 [128, 3, 64, 128, 128], P('slab', None, 'blk'), may hold values from -6 to 6
- integrals: bfloat16 [128, 3, 1200, 1200], P(('slab', 'blk')), may hold values from -0.015625 to 0.015625
- slot_tile: int32 [64], replicated, may hold values from -1 to 99, as said below
Outputs:
- residual: float32 [3, 64, 128, 128], P(None, 'blk', 'slab')
The draws below stay inside these ranges and needn't reach their ends.
Inputs may be any that keep to these rules, and one draw needn't show every extreme that they name: `slot_tile`: each of the 55 block pairs x * 10 + y with x <= y is named by exactly one slot; every other slot holds -1.
All inputs are finite; a program needn't handle non-finite values.
Results may differ from the reference program's by a relative error of at most 0.0003.
Values may be sent and summed in bfloat16 or wider, within the bound.
No kernel may reach another device: no remote copies, remote signals or barrier semaphores. Data moves between devices by JAX's collectives and lax.ppermute only.
A program may use at most 128 MiB of HBM per device.

```python
import jax
import jax.numpy as jnp
import numpy as np
from jax import lax

V = 1200
TILE = 128
NOUT = 3
K = 128
VB = 10
VP = 1280
NTILE = 55
SLOTS = 64


def draw_slot_tile(key, part):
    listing = [x_blk * VB + y_blk for x_blk in range(VB) for y_blk in range(x_blk, VB)]
    listing = listing + [-1] * (SLOTS - NTILE)
    table = jnp.asarray(np.array(listing, dtype=np.int32))
    placing = jax.random.permutation(key, SLOTS)
    return jnp.zeros((SLOTS,), jnp.int32).at[placing].set(table).astype(jnp.int32)


def block_scale(own_key, shape, split, least, largest):
    loudness, own = 1.0, jax.random.fold_in(own_key, 6)
    for axis_at, shards_of in split:
        heights = jnp.exp(jax.random.uniform(jax.random.fold_in(own, axis_at), (shards_of,), jnp.float32, least / len(split), largest / len(split)))
        loudness = loudness * jnp.repeat(heights, shape[axis_at] // shards_of).reshape([-1 if axis == axis_at else 1 for axis in range(len(shape))])
    return loudness


def bell_draw(rng, shape, spread, limit, cuts=(), kind=jnp.bfloat16):
    factor_of = block_scale(rng, shape, cuts, -0.22, 0.18) if cuts else 1.0
    drawn = jax.random.normal(rng, shape, jnp.float32) * spread * factor_of
    return jnp.minimum(jnp.maximum(drawn, -limit), limit).astype(kind)


def setup_inputs(seed: int = 0) -> dict:
    key_list = jax.random.split(jax.random.key(seed), 4)
    amplitudes = bell_draw(key_list[0], (K, NOUT, SLOTS, TILE, TILE), 1.0, 6.0, ((0, 4), (2, 32)))
    integrals = bell_draw(key_list[1], (K, NOUT, V, V), (K * V) ** -0.5, 0.015625, ((0, 128),))
    slot_tile = draw_slot_tile(jax.random.fold_in(key_list[3], 71), 0)
    return dict(amplitudes=amplitudes, integrals=integrals, slot_tile=slot_tile)


def strict_upper(tile_len):
    row_ids = jnp.arange(tile_len)[:, None]
    col_ids = jnp.arange(tile_len)[None, :]
    return row_ids < col_ids


def unpack(packed, slot_tile):
    tile_ids = jnp.arange(VB * VB, dtype=jnp.int32)
    matches = slot_tile[None, :] == tile_ids[:, None]
    slot_ids = jnp.arange(SLOTS, dtype=jnp.int32)[None, :]
    slot_of = jnp.sum(jnp.where(matches, slot_ids, 0), axis=1).astype(jnp.int32)
    present = jnp.any(matches, axis=1)
    tiles = jnp.where(present[:, None, None], packed[slot_of], jnp.zeros((), packed.dtype))
    on_diag = (tile_ids // VB) == (tile_ids % VB)
    keeping = jnp.logical_or(jnp.logical_not(on_diag)[:, None, None], strict_upper(TILE)[None])
    tiles = jnp.where(keeping, tiles, jnp.zeros((), packed.dtype))
    whole = tiles.reshape(VB, VB, TILE, TILE).transpose(0, 2, 1, 3).reshape(VP, VP)
    return (whole - whole.T)[:V, :V]


def reference(amplitudes, integrals, slot_tile):
    ordered = [(source, target) for source in range(NOUT) for target in range(NOUT) if source != target]

    def advance(carry, inputs):
        amp_slab, int_slab = inputs
        fulls = [unpack(amp_slab[source], slot_tile) for source in range(NOUT)]
        updated = tuple(
            carry[number] + jnp.dot(fulls[pair[0]], int_slab[pair[1]], preferred_element_type=jnp.float32)
            for number, pair in enumerate(ordered)
        )
        return updated, None

    initial = tuple(jnp.zeros((V, V), jnp.float32) for entry in ordered)
    sums = lax.scan(advance, initial, (amplitudes, integrals))[0]
    lookup = {pair: number for number, pair in enumerate(ordered)}
    safe_ids = jnp.clip(slot_tile, 0, VB * VB - 1).astype(jnp.int32)
    present = (slot_tile >= 0)[:, None, None]
    results = []
    for source in range(NOUT):
        for target in range(source + 1, NOUT):
            differ = sums[lookup[(source, target)]] - sums[lookup[(target, source)]]
            resid = differ - differ.T
            padded = jnp.pad(resid, ((0, VP - V), (0, VP - V)))
            tiles = padded.reshape(VB, TILE, VB, TILE).transpose(0, 2, 1, 3).reshape(VB * VB, TILE, TILE)
            results.append(jnp.where(present, tiles[safe_ids], jnp.zeros((), jnp.float32)))
    return jnp.stack(results).astype(jnp.float32)
```

```python
import jax
import jax.numpy as jnp
from jax import lax
from jax.experimental import pallas as pl
from jax.experimental.pallas import tpu as pltpu
from jax.sharding import PartitionSpec as P


T = 128
NB = 10
VP = T * NB
V = 1200
LAST = V - (NB - 1) * T
BLOCKS = [(x, y) for x in range(NB) for y in range(x, NB)]
NUMBER = {pair: n for n, pair in enumerate(BLOCKS)}
SLOTS = 64
EMPTY = SLOTS - len(BLOCKS)
PIECES = 132
F32 = jnp.float32
BF16 = jnp.bfloat16
WHOLE = pl.BlockSpec(memory_space=pltpu.VMEM)
SCALARS = pl.BlockSpec(memory_space=pltpu.SMEM)


def slot_table(slot_tile, x, y, z, core):
    ids = jnp.arange(SLOTS, dtype=jnp.int32)
    before = jnp.logical_or(
        slot_tile[None, :] < slot_tile[:, None],
        jnp.logical_and(slot_tile[None, :] == slot_tile[:, None], ids[None, :] < ids[:, None]),
    )
    rank = jnp.sum(before.astype(jnp.int32), axis=1)
    order = jnp.sum(jnp.where(rank[None, :] == ids[:, None], ids[None, :], 0), axis=1)
    parity = order & 1
    other = ((order >> 1) & 1) ^ core
    dz = (((order >> 2) & 3) - z) & 3
    dy = ((order >> 4) - y) & 3
    base = parity * 64 + jnp.where(parity == 0, dy * 4 + dz, dy * 16 + dz * 4)
    stride = jnp.where(parity == 0, 16, 1)
    mine = jnp.where(other == 0, base, 128)
    mine_stride = jnp.where(other == 0, stride, 1)
    theirs = jnp.where(other == 1, base, 128)
    theirs_stride = jnp.where(other == 1, stride, 1)
    steps = (ids - x) & 3
    return jnp.concatenate([order, mine, mine_stride, theirs, theirs_stride, steps]).astype(jnp.int32)


def unpack_body(count, table, raw, *outs):
    rows = lax.broadcasted_iota(jnp.int32, (T, T), 0)
    cols = lax.broadcasted_iota(jnp.int32, (T, T), 1)
    for number in range(count):
        out = outs[number]
        for n, (x, y) in enumerate(BLOCKS):
            slot = table[EMPTY + n]
            tile = raw[slot >> 1, number, slot & 1].astype(F32)
            keep = None
            if x == y:
                keep = rows < cols
            if y == NB - 1:
                inside = cols < LAST
                keep = inside if keep is None else jnp.logical_and(keep, inside)
            if keep is not None:
                tile = jnp.where(keep, tile, 0.0)
            if x == y:
                out[x * T : (x + 1) * T, y * T : (y + 1) * T] = (tile - tile.T).astype(BF16)
            else:
                out[x * T : (x + 1) * T, y * T : (y + 1) * T] = tile.astype(BF16)
                out[y * T : (y + 1) * T, x * T : (x + 1) * T] = (-tile.T).astype(BF16)


def unpack(table, raw):
    count = raw.shape[1]
    return pl.pallas_call(
        lambda *refs: unpack_body(count, *refs),
        out_shape=[jax.ShapeDtypeStruct((VP, VP), BF16)] * count,
        in_specs=[SCALARS, WHOLE],
        out_specs=[WHOLE] * count,
        name="unpack",
    )(table, raw)


def tri_body(signs, started, packing, table, *refs):
    count = len(signs)
    lefts, rights = refs[:count], refs[count : 2 * count]
    rest = refs[2 * count :]
    start = rest[0] if started else None
    outs = rest[1:] if started else rest

    def put(number, tile):
        for g in range(4):
            piece = tile[32 * g : 32 * g + 32]
            step = table[5 * SLOTS + g]
            outs[0][table[SLOTS + number] + step * table[2 * SLOTS + number]] = piece
            outs[1][table[3 * SLOTS + number] + step * table[4 * SLOTS + number]] = piece

    if packing:
        for number in range(EMPTY):
            put(number, jnp.zeros((T, T), F32))
    wide = 2 * T
    for i in range(NB // 2):
        total = None
        for sign, left, right in zip(signs, lefts, rights):
            part = jnp.dot(
                left[i * wide : (i + 1) * wide, :], right[:, i * wide :], preferred_element_type=F32
            )
            if total is None:
                total = part if sign > 0 else -part
            else:
                total = total + part if sign > 0 else total - part
        for x in (2 * i, 2 * i + 1):
            for y in range(x, NB):
                n = NUMBER[x, y]
                top, side = (x - 2 * i) * T, (y - 2 * i) * T
                tile = total[top : top + T, side : side + T]
                if started:
                    tile = tile + start[n]
                if packing:
                    put(EMPTY + n, tile)
                else:
                    outs[0][n] = tile


def tri(table, terms, start=None, packing=True):
    signs = tuple(sign for sign, _, _ in terms)
    operands = [left for _, left, _ in terms] + [right for _, _, right in terms]
    if start is not None:
        operands.append(start)
    if packing:
        shapes = [jax.ShapeDtypeStruct((PIECES, 32, T), F32)] * 2
    else:
        shapes = [jax.ShapeDtypeStruct((len(BLOCKS), T, T), F32)]
    return pl.pallas_call(
        lambda *refs: tri_body(signs, start is not None, packing, *refs),
        out_shape=shapes,
        in_specs=[SCALARS] + [WHOLE] * len(operands),
        out_specs=[WHOLE] * len(shapes),
        cost_estimate=pl.CostEstimate(
            flops=2 * VP * VP * VP * 6 // 10 * len(terms), transcendentals=0, bytes_accessed=20_000_000
        ),
        name="tri",
    )(table, *operands)


def local(amplitudes, integrals, slot_tile):
    x = lax.axis_index("slab")
    blk = lax.axis_index("blk")
    y, z, core = blk >> 3, (blk >> 1) & 3, blk & 1
    axes = ("slab", "blk")
    places = [(a, b, c, d) for a in range(4) for b in range(4) for c in range(4) for d in range(2)]

    def flat(a, b, c, d):
        return (a % 4) * 32 + (b % 4) * 8 + (c % 4) * 2 + d % 2

    def shifted(value, da, db, dc, dd):
        pairs = [(flat(a, b, c, d), flat(a + da, b + db, c + dc, d + dd)) for a, b, c, d in places]
        return lax.ppermute(value, axes, pairs)

    shifts = {
        "x": lambda value, by: shifted(value, by, 0, 0, 0),
        "y": lambda value, by: shifted(value, 0, by, 0, 0),
        "z": lambda value, by: shifted(value, 0, 0, by, 0),
    }

    def reduced(value, axis):
        total = value[0]
        for by in range(1, 4):
            total = total + shifts[axis](value[by], by)
        return total

    def move(part):
        return lax.all_to_all(part, "blk", split_axis=0, concat_axis=0, tiled=True)

    raw01 = move(amplitudes[:, :2])
    raw2 = move(amplitudes[:, 2:])
    table = slot_table(slot_tile, x, y, z, core)
    pad = VP - V
    w = [jnp.pad(integrals[0, q], ((0, pad), (0, pad))) for q in range(3)]
    wt = [jnp.swapaxes(each, 0, 1) for each in w]
    f0, f1 = unpack(table, raw01)
    r01 = tri(table, [(1, f0, w[1]), (1, wt[1], f0), (-1, f1, w[0]), (-1, wt[0], f1)])
    (a02,) = tri(table, [(1, f0, w[2]), (1, wt[2], f0)], packing=False)
    (a12,) = tri(table, [(1, f1, w[2]), (1, wt[2], f1)], packing=False)
    (f2,) = unpack(table, raw2)
    r02 = tri(table, [(-1, f2, w[0]), (-1, wt[0], f2)], start=a02)
    r12 = tri(table, [(-1, f2, w[1]), (-1, wt[1], f2)], start=a12)

    def first(pair):
        mine, theirs = pair
        got = shifted(theirs, 0, 0, 0, 1)
        both = (mine[:128] + got[:128]).reshape(2, 4, 16, 32, T)
        return reduced(both[0], "x"), reduced(both[1], "y")

    firsts = [first(pair) for pair in (r01, r02, r12)]
    outs = []
    for group in ((0,), (1, 2)):
        even = jnp.stack([firsts[g][0] for g in group], axis=1).reshape(4, 4, len(group), 32, T)
        odd = jnp.stack([firsts[g][1] for g in group], axis=1).reshape(4, 4, len(group), 32, T)
        even = reduced(reduced(even, "y"), "z")
        odd = reduced(reduced(odd, "z"), "x")
        outs.append(jnp.stack([even, odd], axis=1))
    return jnp.concatenate(outs, axis=0)


def solution(mesh):
    return jax.shard_map(
        local,
        mesh=mesh,
        in_specs=(P("slab", None, "blk", None, None), P(("slab", "blk"), None, None, None), P()),
        out_specs=P(None, "blk", "slab", None),
        check_vma=False,
    )
```
